32 devices in a mesh: dp: 2 (over x), b: 4 (over z), cp: 4 (over y, core).
Axes of the slice: x: 2, y: 2, z: 4, core: 2. Of those that a mesh axis runs over, the one named last changes fastest.
Arguments:
- x: bfloat16 [8, 4096, 2048], P(('dp', 'b'), 'cp'), parts along dimension 0
- ids: int32 [8, 4096, 6], P(('dp', 'b'), 'cp'), parts along dimension 0
- g_attn: bfloat16 [2048], replicated
- w_q: bfloat16 [2048, 3072], replicated
- w_dkv: bfloat16 [2048, 512], replicated
- w_kr: bfloat16 [2048, 64], replicated
- w_uk: bfloat16 [16, 128, 512], replicated
- w_uv: bfloat16 [16, 512, 128], replicated
- w_o: bfloat16 [2048, 2048], replicated
- g_ffn: bfloat16 [2048], replicated
- w_fg: bfloat16 [2048, 10944], replicated
- w_fu: bfloat16 [2048, 10944], replicated
- w_fd: bfloat16 [10944, 2048], replicated
- g_moe: bfloat16 [2048], replicated
- w_r: bfloat16 [2048, 96], replicated
- w_eg: bfloat16 [64, 2048, 1408], P(('b', 'cp'))
- w_eu: bfloat16 [64, 2048, 1408], P(('b', 'cp'))
- w_ed: bfloat16 [64, 1408, 2048], P(('b', 'cp'))
Outputs:
- output: bfloat16 [8, 4096, 2048], P(('dp', 'b'), 'cp'), parts along dimension 0
There are 2 independent parts. The reference program is written for one: setup_inputs(seed, part) draws one part's arguments, and reference() takes and returns one part's arrays. A program takes and returns all parts, laid end to end along the dimension named above; an argument that names none is the same for every part.
All inputs are finite; a program needn't handle non-finite values.
Results may differ from the reference program's by a relative error of at most 0.0088785.
Values are sent between devices in bfloat16 or wider.
A program may use at most 1 GiB of HBM per device.

```python
import jax
import jax.numpy as jnp
from jax import lax

D = 2048
HEADS = 16
R = 512
EXPERTS = 64
TOP = 6
EFF = 1408
FF = 10944
ROWS = 1
SEQ = 1024
NB = 4
NC = 4
NOPE = 128
ROPE = 64
VDIM = 128

B = ROWS * NB
S = SEQ * NC
T = B * S
TBLK = ROWS * SEQ
NSLOT = EXPERTS + EXPERTS // 2
WIDTH = NSLOT // TOP
HOT = WIDTH // 2
CAP = (TBLK + HOT - 1) // HOT
CAPALL = NB * NC * CAP
EPS = 1e-6
SCALE = (NOPE + ROPE) ** -0.5


def _nrm(k, shape, scale):
    return (jax.random.normal(k, shape, jnp.float32) * scale).astype(jnp.bfloat16)


def _gain(k):
    return jax.random.uniform(k, (D,), jnp.float32, 0.6, 1.4).astype(jnp.bfloat16)


def setup_inputs(seed: int = 0, part: int = 0) -> dict:
    kp = jax.random.fold_in(jax.random.key(seed), part)
    kw = jax.random.split(jax.random.key(seed + 1), 16)
    k1, k2, k3, k4, k5 = jax.random.split(kp, 5)
    pos = jnp.arange(S, dtype=jnp.float32) / S
    amp = jax.random.normal(k2, (B, 3, D), jnp.float32) * 0.6
    phase = jax.random.uniform(k3, (B, 3, 1), jnp.float32, 0.0, 6.2832)
    freq = jnp.arange(1, 4, dtype=jnp.float32).reshape(1, 3, 1)
    wave = jnp.cos(6.2832 * freq * pos.reshape(1, 1, S) + phase)
    x = 0.7 * jax.random.normal(k1, (B, S, D), jnp.float32) + jnp.einsum('clt,cle->cte', wave, amp)
    ka, kb, kc = jax.random.split(jax.random.fold_in(kp, 7), 3)
    shift = jax.random.randint(ka, (), 0, NSLOT)
    perm = (jnp.arange(NSLOT) + shift) % NSLOT
    tperm = jax.vmap(lambda kk: jax.random.permutation(kk, TBLK))(jax.random.split(kb, NB * NC * TOP))
    off = jax.random.randint(kc, (NB * NC * TOP, 1), 0, WIDTH - HOT + 1)
    r = (tperm % HOT + off).reshape(NB, NC, TOP, TBLK)
    slot = jnp.arange(TOP).reshape(1, 1, TOP, 1) * WIDTH + r
    ids = perm[slot].reshape(NB, NC, TOP, ROWS, SEQ).transpose(0, 3, 1, 4, 2).reshape(B, S, TOP)
    return {
        'x': x.astype(jnp.bfloat16),
        'ids': ids.astype(jnp.int32),
        'g_attn': _gain(kw[0]),
        'w_q': _nrm(kw[1], (D, HEADS * (NOPE + ROPE)), D ** -0.5),
        'w_dkv': _nrm(kw[2], (D, R), D ** -0.5),
        'w_kr': _nrm(kw[3], (D, ROPE), D ** -0.5),
        'w_uk': _nrm(kw[4], (HEADS, NOPE, R), 0.5 * NOPE ** -0.5),
        'w_uv': _nrm(kw[5], (HEADS, R, VDIM), R ** -0.5),
        'w_o': _nrm(kw[6], (HEADS * VDIM, D), (HEADS * VDIM) ** -0.5),
        'g_ffn': _gain(kw[7]),
        'w_fg': _nrm(kw[8], (D, FF), D ** -0.5),
        'w_fu': _nrm(kw[9], (D, FF), D ** -0.5),
        'w_fd': _nrm(kw[10], (FF, D), FF ** -0.5),
        'g_moe': _gain(kw[11]),
        'w_r': _nrm(kw[12], (D, NSLOT), 2.0 * D ** -0.5),
        'w_eg': _nrm(kw[13], (EXPERTS, D, EFF), D ** -0.5),
        'w_eu': _nrm(kw[14], (EXPERTS, D, EFF), D ** -0.5),
        'w_ed': _nrm(kw[15], (EXPERTS, EFF, D), 2.0 * EFF ** -0.5),
    }


def _rms(v, g):
    vf = v.astype(jnp.float32)
    return (vf * lax.rsqrt(jnp.mean(vf * vf, axis=-1, keepdims=True) + EPS) * g.astype(jnp.float32)).astype(jnp.bfloat16)


def _rope(v, cos, sin):
    half = ROPE // 2
    v1 = v[..., :half]
    v2 = v[..., half:]
    return jnp.concatenate([v1 * cos - v2 * sin, v1 * sin + v2 * cos], axis=-1)


def _swiglu(z, wg, wu, wd):
    hid = jax.nn.silu(jnp.dot(z, wg, preferred_element_type=jnp.float32)) * jnp.dot(z, wu, preferred_element_type=jnp.float32)
    return jnp.dot(hid.astype(jnp.bfloat16), wd, preferred_element_type=jnp.float32).astype(jnp.bfloat16)


def reference(x, ids, g_attn, w_q, w_dkv, w_kr, w_uk, w_uv, w_o, g_ffn, w_fg, w_fu, w_fd, g_moe, w_r, w_eg, w_eu, w_ed):
    pos = jnp.arange(S)
    half = ROPE // 2
    ang = pos.astype(jnp.float32)[:, None] * (10000.0 ** (-jnp.arange(half, dtype=jnp.float32) / half))[None, :]
    cos = jnp.cos(ang)
    sin = jnp.sin(ang)
    causal = pos[:, None] >= pos[None, :]

    def attn_row(xr):
        n = _rms(xr, g_attn)
        c = jnp.dot(n, w_dkv, preferred_element_type=jnp.float32).astype(jnp.bfloat16)
        kr = _rope(jnp.dot(n, w_kr, preferred_element_type=jnp.float32), cos, sin).astype(jnp.bfloat16)
        q = jnp.dot(n, w_q, preferred_element_type=jnp.float32).reshape(S, HEADS, NOPE + ROPE)
        qn = q[..., :NOPE].astype(jnp.bfloat16)
        qt = jnp.einsum('shn,hnr->shr', qn.astype(jnp.float32), w_uk.astype(jnp.float32)).astype(jnp.bfloat16)
        qr = _rope(q[..., NOPE:], cos[:, None, :], sin[:, None, :]).astype(jnp.bfloat16)

        def head(hargs):
            qh, qrh, wuv = hargs
            sc = (jnp.dot(qh, c.T, preferred_element_type=jnp.float32) + jnp.dot(qrh, kr.T, preferred_element_type=jnp.float32)) * SCALE
            sc = jnp.where(causal, sc, -jnp.inf)
            p = jnp.exp(sc - jnp.max(sc, axis=-1, keepdims=True))
            lat = (jnp.dot(p.astype(jnp.bfloat16), c, preferred_element_type=jnp.float32) / jnp.sum(p, axis=-1, keepdims=True)).astype(jnp.bfloat16)
            return jnp.dot(lat, wuv, preferred_element_type=jnp.float32).astype(jnp.bfloat16)

        o = lax.map(head, (jnp.transpose(qt, (1, 0, 2)), jnp.transpose(qr, (1, 0, 2)), w_uv))
        o = jnp.transpose(o, (1, 0, 2)).reshape(S, HEADS * VDIM)
        return jnp.dot(o, w_o, preferred_element_type=jnp.float32).astype(jnp.bfloat16)

    a = lax.map(attn_row, x)
    y = (x.astype(jnp.float32) + a.astype(jnp.float32)).astype(jnp.bfloat16)
    n2 = _rms(y, g_ffn).reshape(B * NC, SEQ, D)
    f = lax.map(lambda z: _swiglu(z, w_fg, w_fu, w_fd), n2).reshape(T, D)
    u = _rms(x, g_moe).reshape(T, D)
    idf = ids.reshape(T, TOP)
    g = jax.nn.softmax(jnp.dot(u, w_r, preferred_element_type=jnp.float32), axis=-1)
    sel = jnp.take_along_axis(g, idf, axis=1)
    gate = sel / jnp.sum(sel, axis=1, keepdims=True)
    gflat = gate.reshape(-1)
    flat = idf.reshape(-1)
    order = jnp.argsort(flat, stable=True)
    starts = jnp.searchsorted(flat[order], jnp.arange(EXPERTS + 1, dtype=flat.dtype))
    zero = jnp.sum(jnp.where(idf >= EXPERTS, gate, 0.0), axis=1)
    m0 = zero[:, None] * u.astype(jnp.float32)

    def expert(m, eargs):
        e, wg, wu, wd = eargs
        k = starts[e] + jnp.arange(CAPALL)
        slot = order[jnp.minimum(k, T * TOP - 1)]
        tok = slot // TOP
        out = _swiglu(u[tok], wg, wu, wd)
        w = jnp.where(k < starts[e + 1], gflat[slot], 0.0)
        return m.at[tok].add(w[:, None] * out.astype(jnp.float32)), None

    m, _ = lax.scan(expert, m0, (jnp.arange(EXPERTS), w_eg, w_eu, w_ed))
    h = y.reshape(T, D).astype(jnp.float32) + f.astype(jnp.float32) + m
    return h.astype(jnp.bfloat16).reshape(B, S, D)
```

```python
import functools

import jax
import jax.numpy as jnp
from jax import lax
from jax.experimental import pallas as pl
from jax.experimental.pallas import tpu as pltpu
from jax.sharding import PartitionSpec as P


F32 = jnp.float32
BF16 = jnp.bfloat16
EPS = 1e-6


NOPE, ROPE = 128, 64
SCALE=(NOPE+ROPE)**-0.5
LOG2E=1.4426950408889634


def _rope(v, c, sa, sb):
    return v*c + pltpu.roll(v, 32, 1)*sa + pltpu.roll(v, 96, 1)*sb


def _pre_body(x_ref, ga_ref, gm_ref, wc_ref, wk_ref, wr_ref, c_ref, sa_ref, sb_ref, n_ref, kv_ref, lg_ref, *u_refs):
    xf = x_ref[...].astype(F32)
    z = xf * lax.rsqrt(jnp.mean(xf*xf, axis=-1, keepdims=True) + EPS)
    n = (z * ga_ref[...].astype(F32)).astype(BF16)
    u = (z * gm_ref[...].astype(F32)).astype(BF16)
    n_ref[...] = n
    w = u.shape[1]//len(u_refs)
    for k, r in enumerate(u_refs): r[...] = u[:, k*w:(k+1)*w]
    r = wc_ref.shape[1]
    kv_ref[:, :r] = jnp.dot(n, wc_ref[...], preferred_element_type=F32).astype(BF16)
    kr = jnp.dot(n, wk_ref[...], preferred_element_type=F32)
    kr = jnp.concatenate([kr, jnp.zeros_like(kr)], axis=1)
    kv_ref[:, r:] = _rope(kr, c_ref[...], sa_ref[...], sb_ref[...]).astype(BF16)
    lg_ref[...] = jnp.dot(u, wr_ref[...], preferred_element_type=F32)


def pre(x, ga, gm, wc, wk, wr, tabs, nk, tm=256):
    t, d = x.shape
    r = wc.shape[1]
    row = lambda w: pl.BlockSpec((tm, w), lambda i: (i, 0))
    full = lambda a: pl.BlockSpec(a.shape, lambda i: (0,)*a.ndim)
    ns = wr.shape[1]
    return pl.pallas_call(_pre_body, grid=(t//tm,),
        in_specs=[row(d), full(ga), full(gm), full(wc), full(wk), full(wr), row(128), row(128), row(128)],
        out_specs=[row(d), row(r+128), row(ns)] + [row(d//nk)]*nk,
        out_shape=[jax.ShapeDtypeStruct((t, d), BF16), jax.ShapeDtypeStruct((t, r+128), BF16), jax.ShapeDtypeStruct((t, ns), F32)]
                  + [jax.ShapeDtypeStruct((t, d//nk), BF16)]*nk,
        name="pre", cost_estimate=pl.CostEstimate(flops=1024, bytes_accessed=6*t*d, transcendentals=0),
        compiler_params=pltpu.CompilerParams(dimension_semantics=("arbitrary",), vmem_limit_bytes=40<<20))(x, ga, gm, wc, wk, wr, *tabs)


def _qproj_body(n_ref, w_ref, uk_ref, c_ref, sa_ref, sb_ref, o_ref):
    q = jnp.dot(n_ref[...], w_ref[...], preferred_element_type=F32)
    t0, t1, t2 = q[:, :128], q[:, 128:256], q[:, 256:]
    r1, r2 = pltpu.roll(t1, 64, 1), pltpu.roll(t2, 64, 1)
    lane = lax.broadcasted_iota(jnp.int32, t0.shape, 1)
    nope = (t0, jnp.where(lane < 64, r1, r2))
    rope = (t1, r2)
    c, sa, sb = c_ref[...], sa_ref[...], sb_ref[...]
    r = uk_ref.shape[2]
    for k in range(2):
        o_ref[k, :, :r] = jnp.dot(nope[k].astype(BF16), uk_ref[k], preferred_element_type=F32).astype(BF16)
        o_ref[k, :, r:] = _rope(rope[k], c, sa, sb).astype(BF16)


def qproj(n, wq, wuk, tabs, tm=512):
    t, d = n.shape
    h, _, r = wuk.shape
    tab = pl.BlockSpec((tm, 128), lambda j, i: (i, 0))
    return pl.pallas_call(_qproj_body, grid=(h//2, t//tm),
        in_specs=[pl.BlockSpec((tm, d), lambda j, i: (i, 0)), pl.BlockSpec((d, 384), lambda j, i: (0, j)),
                  pl.BlockSpec((2, NOPE, r), lambda j, i: (j, 0, 0)), tab, tab, tab],
        out_specs=pl.BlockSpec((2, tm, r+128), lambda j, i: (j, i, 0)),
        out_shape=jax.ShapeDtypeStruct((h, t, r+128), BF16), name="qproj",
        cost_estimate=pl.CostEstimate(flops=1024, bytes_accessed=2*(h//2*t*d+d*h*192+t*h*(r+128)), transcendentals=0),
        compiler_params=pltpu.CompilerParams(dimension_semantics=("arbitrary","arbitrary"), vmem_limit_bytes=40<<20))(n, wq, wuk, *tabs)


def _attn_body(tq, sub, i_ref, q_ref, k0, k1, k2, k3, uv_ref, o_ref, m_ref, l_ref, acc_ref):
    at = i_ref[0]
    seq, r = q_ref.shape[1], uv_ref.shape[1]
    CF = SCALE*LOG2E
    nt = (((1,), (1,)), ((), ()))
    def block(rows, kv, diag, first):
        q = q_ref[0, rows:rows+sub]
        s = lax.dot_general(q, kv, nt, preferred_element_type=F32)
        if diag is not None:
            rr = lax.broadcasted_iota(jnp.int32, s.shape, 0) + diag
            cc = lax.broadcasted_iota(jnp.int32, s.shape, 1)
            s = jnp.where(rr >= cc, s, -jnp.inf)
        mx = jnp.max(s, axis=1, keepdims=True)
        if first:
            m = jnp.broadcast_to(mx, (sub, 128))
            p = jnp.exp2((s - mx)*CF)
            l_ref[rows:rows+sub] = jnp.broadcast_to(jnp.sum(p, axis=1, keepdims=True), (sub, 128))
            acc_ref[rows:rows+sub] = jnp.dot(p.astype(BF16), kv[:, :r], preferred_element_type=F32)
        else:
            m0 = m_ref[rows:rows+sub]
            m = jnp.maximum(m0, mx)
            corr = jnp.exp2((m0 - m)*CF)
            p = jnp.exp2((s - m[:, :1])*CF)
            l_ref[rows:rows+sub] = l_ref[rows:rows+sub]*corr + jnp.sum(p, axis=1, keepdims=True)
            acc_ref[rows:rows+sub] = acc_ref[rows:rows+sub]*corr[:, :1] + jnp.dot(p.astype(BF16), kv[:, :r], preferred_element_type=F32)
        m_ref[rows:rows+sub] = m
    for t0 in range(0, seq, tq):
        for rows in range(t0, t0+tq, sub):
            block(rows, k0[:t0+tq], rows, True)
    for ok, kr in ((at >= 2, k1), (lax.rem(at, 2) == 1, k2), (at >= 2, k3)):
        @pl.when(ok)
        def _():
            for rows in range(0, seq, sub):
                block(rows, kr[...], None, False)
    for rows in range(0, seq, 256):
        lat = (acc_ref[rows:rows+256] / l_ref[rows:rows+256, :1]).astype(BF16)
        o_ref[rows:rows+256] = jnp.dot(lat, uv_ref[0], preferred_element_type=F32).astype(BF16)


def attn(i, q, kvs, wuv, part, parts, tq=512, sub=512):
    h, t, w = q.shape
    r, vd = wuv.shape[1:]
    hp = h // parts
    o = part * hp
    kspec = pl.BlockSpec((t, w), lambda j, *_: (0, 0), pipeline_mode=pl.Buffered(1))
    return pl.pallas_call(functools.partial(_attn_body, tq, sub),
        grid_spec=pltpu.PrefetchScalarGridSpec(num_scalar_prefetch=1, grid=(hp,),
            in_specs=[pl.BlockSpec((1, t, w), lambda j, *_: (j + o, 0, 0)), kspec, kspec, kspec, kspec,
                      pl.BlockSpec((1, r, vd), lambda j, *_: (j + o, 0, 0))],
            out_specs=pl.BlockSpec((t, vd), lambda j, *_: (0, j)),
            scratch_shapes=[pltpu.VMEM((t, 128), F32), pltpu.VMEM((t, 128), F32), pltpu.VMEM((t, r), F32)]),
        out_shape=jax.ShapeDtypeStruct((t, hp*vd), BF16), name="attn",
        cost_estimate=pl.CostEstimate(flops=1024, bytes_accessed=2*hp*t*w, transcendentals=hp*t*t*5//2),
        compiler_params=pltpu.CompilerParams(dimension_semantics=("arbitrary",), vmem_limit_bytes=60<<20))(i, q, *kvs, wuv)


def _pick_body(h_ref, rank_ref, u_ref, o_ref):
    ne, cap = o_ref.shape[0], o_ref.shape[2]
    t = u_ref.shape[1]
    row = lax.broadcasted_iota(jnp.int32, (cap, t), 0)
    oh = jnp.concatenate([(rank_ref[0, e:e+1, :] == row).astype(F32).astype(BF16) for e in range(ne)], axis=0)
    o = jnp.dot(oh, u_ref[0], preferred_element_type=F32).astype(BF16)
    for e in range(ne):
        o_ref[e, 0] = o[e*cap:(e+1)*cap]


def pick(h, rank, u, nl, cap):
    _, E, t = rank.shape
    d = u.shape[-1]
    return pl.pallas_call(
        _pick_body,
        grid_spec=pltpu.PrefetchScalarGridSpec(num_scalar_prefetch=1, grid=(nl,),
            in_specs=[pl.BlockSpec((1, E, t), lambda s, h: (h[0] + s, 0, 0)), pl.BlockSpec((1, t, d), lambda s, h: (h[1] + s, 0, 0))],
            out_specs=pl.BlockSpec((E, 1, cap, d), lambda s, h: (0, s, 0, 0))),
        out_shape=jax.ShapeDtypeStruct((E, nl, cap, d), BF16), name="pick",
        cost_estimate=pl.CostEstimate(flops=1024, bytes_accessed=2*nl*(t+E*cap)*d, transcendentals=0),
        compiler_params=pltpu.CompilerParams(dimension_semantics=("arbitrary",), vmem_limit_bytes=40<<20))(h, rank, u)


def _expert_body(e0, ne, n_ref, lst_ref, x_hbm, wg_hbm, wu_hbm, wd_hbm, o_hbm,
                 x_ref, w_ref, wd_ref, hid_ref, f_ref, ob_ref, xsem, wsem, dsem, osem):
    _, S, cap, d = x_hbm.shape
    ff = wg_hbm.shape[-1]
    kc = d // 4
    half = S // 2
    tm = half * cap
    def wcopies(e):
        b = e % 2
        out = []
        for i in range(4):
            out.append(pltpu.make_async_copy(wg_hbm.at[e, pl.ds(i*kc, kc)], w_ref.at[b, pl.ds(i*kc, kc), pl.ds(0, ff)], wsem.at[b, 0, i]))
            out.append(pltpu.make_async_copy(wu_hbm.at[e, pl.ds(i*kc, kc)], w_ref.at[b, pl.ds(i*kc, kc), pl.ds(ff, ff)], wsem.at[b, 1, i]))
        return out
    def dcopy(e):
        return pltpu.make_async_copy(wd_hbm.at[e], wd_ref.at[e % 2], dsem.at[e % 2])
    def xcopies(e):
        return [pltpu.make_async_copy(x_hbm.at[e, lst_ref[e*S + j]], x_ref.at[e % 2, pl.ds(j*cap, cap)], xsem.at[e % 2, j]) for j in range(S)]
    def ocopies(e, m):
        out = []
        for j in range(half):
            s = lst_ref[e*S + m*half + j]
            out.append(pltpu.make_async_copy(ob_ref.at[m, pl.ds(j*cap*16, cap*16)], o_hbm.at[pl.ds((s*ne + e - e0)*cap*16, cap*16)], osem.at[m, j]))
        return out
    def when(e, m):
        return n_ref[e] > m*half
    def load(e):
        @pl.when(when(e, 0))
        def _():
            for c in wcopies(e): c.start()
            for c in xcopies(e): c.start()
            dcopy(e).start()
    def out_wait(e, m):
        @pl.when(when(e, m))
        def _():
            for c in ocopies(e, m): c.wait()
    load(e0)
    for e in range(e0, e0 + ne):
        b = e % 2
        if e + 1 < e0 + ne:
            load(e + 1)
        @pl.when(when(e, 0))
        def _():
            for c in xcopies(e): c.wait()
            for c in wcopies(e): c.wait()
        for m in range(2):
            if e > e0:
                out_wait(e - 1, m)
            @pl.when(when(e, m))
            def _():
                gu = jnp.dot(x_ref[b, m*tm:(m+1)*tm], w_ref[b], preferred_element_type=F32)
                g, u = gu[:, :ff], gu[:, ff:]
                hid_ref[...] = (g * jax.nn.sigmoid(g) * u).astype(BF16)
                if m == 0:
                    dcopy(e).wait()
                for c0 in range(0, d, 1024):
                    o = jnp.dot(hid_ref[...], wd_ref[b, :, c0:c0+1024], preferred_element_type=F32)
                    for k in range(0, 1024, 128):
                        f_ref[pl.ds((c0+k)//128, tm, stride=16), :] = o[:, k:k+128]
                ob_ref[m] = f_ref[...].astype(BF16)
                for c in ocopies(e, m): c.start()
    for m in range(2):
        out_wait(e0 + ne - 1, m)


def expert(e0, ne, n, lst, xg, wg, wu, wd):
    E, S, cap, d = xg.shape
    ff = wg.shape[-1]
    tm = S // 2 * cap
    any_ = pl.BlockSpec(memory_space=pl.ANY)
    return pl.pallas_call(
        functools.partial(_expert_body, e0, ne),
        grid_spec=pltpu.PrefetchScalarGridSpec(num_scalar_prefetch=2, grid=(), in_specs=[any_]*4, out_specs=any_,
            scratch_shapes=[pltpu.VMEM((2, S*cap, d), BF16), pltpu.VMEM((2, d, 2*ff), BF16), pltpu.VMEM((2, ff, d), BF16),
                            pltpu.VMEM((tm, ff), BF16), pltpu.VMEM((tm*16, 128), F32), pltpu.VMEM((2, tm*16, 128), BF16),
                            pltpu.SemaphoreType.DMA((2, S)), pltpu.SemaphoreType.DMA((2, 2, 4)), pltpu.SemaphoreType.DMA((2,)),
                            pltpu.SemaphoreType.DMA((2, S//2))]),
        out_shape=jax.ShapeDtypeStruct((S*ne*cap*16, 128), BF16), name="expert",
        cost_estimate=pl.CostEstimate(flops=1024, bytes_accessed=6*E*d*ff+4*E*S*cap*d, transcendentals=E*S*cap*ff),
        compiler_params=pltpu.CompilerParams(vmem_limit_bytes=62<<20))(n, lst, xg, wg, wu, wd)


def _rows(k_ref, idx_ref, w_ref, r_refs, buf, scr, sem, tt):
    n = buf.shape[0] - 16
    m = n // len(r_refs)
    i = pl.program_id(0)
    t = pl.num_programs(0)*tt
    @pl.when(i == 0)
    def _():
        cs = [pltpu.make_async_copy(r, buf.at[pl.ds(c*m, m)], sem.at[c]) for c, r in enumerate(r_refs)]
        for c in cs: c.start()
        buf[n:n+16] = jnp.zeros((16, 128), BF16)
        for c in cs: c.wait()
    def row(j, q):
        g = j*t + i*tt + q
        return w_ref[g]*buf[pl.ds(pl.multiple_of(idx_ref[g]*16, 16), 16), :].astype(F32)
    def first(q, _):
        scr[pl.ds(pl.multiple_of(q*16, 16), 16), :] = row(0, q)
        return 0
    lax.fori_loop(0, tt, first, 0, unroll=8)
    def more(j, _):
        def add(q, _):
            s = pl.ds(pl.multiple_of(q*16, 16), 16)
            scr[s, :] = scr[s, :] + row(j, q)
            return 0
        lax.fori_loop(0, tt, add, 0, unroll=8)
        return 0
    lax.fori_loop(1, k_ref[0], more, 0)


def _part_body(nr, k_ref, idx_ref, w_ref, *rest):
    r_refs, (*prev, o_ref, buf, sem) = rest[:nr], rest[nr:]
    _rows(k_ref, idx_ref, w_ref, r_refs, buf, o_ref, sem, o_ref.shape[0]//16)
    for p in prev:
        o_ref[...] += p[...]


def part(k, idx, w, rets, prev, t, tt=128):
    n = sum(r.shape[0] for r in rets)
    blk = pl.BlockSpec((tt*16, 128), lambda i, *_: (i, 0))
    return pl.pallas_call(functools.partial(_part_body, len(rets)),
        grid_spec=pltpu.PrefetchScalarGridSpec(num_scalar_prefetch=3, grid=(t//tt,),
            in_specs=[pl.BlockSpec(memory_space=pl.ANY)]*len(rets) + [blk]*len(prev), out_specs=blk,
            scratch_shapes=[pltpu.VMEM((n+16, 128), BF16), pltpu.SemaphoreType.DMA((len(rets),))]),
        out_shape=jax.ShapeDtypeStruct((t*16, 128), F32), name="part",
        cost_estimate=pl.CostEstimate(flops=1024, bytes_accessed=2*n*128+12*t*2048, transcendentals=0),
        compiler_params=pltpu.CompilerParams(dimension_semantics=("arbitrary",), vmem_limit_bytes=40<<20))(k, idx, w, *rets, *prev)


def _final_body(nr, k_ref, idx_ref, w_ref, z_ref, y_ref, f_ref, u_ref, *rest):
    r_refs, (*prev, h_ref, buf, scr, sem) = rest[:nr], rest[nr:]
    tt = y_ref.shape[0]
    _rows(k_ref, idx_ref, w_ref, r_refs, buf, scr, sem, tt)
    for p in prev:
        scr[...] += p[...]
    z = z_ref[...]
    for k in range(16):
        c = slice(k*128, (k+1)*128)
        m = scr[pl.ds(k, tt, stride=16), :] + z*u_ref[:, c].astype(F32)
        h_ref[:, c] = (y_ref[:, c].astype(F32) + f_ref[:, c].astype(F32) + m).astype(BF16)


def final(k, idx, w, rets, zero, y, f, u, prev, tt=128):
    t, d = y.shape
    n = sum(r.shape[0] for r in rets)
    row = lambda c: pl.BlockSpec((tt, c), lambda i, *_: (i, 0))
    blk = pl.BlockSpec((tt*16, 128), lambda i, *_: (i, 0))
    return pl.pallas_call(functools.partial(_final_body, len(rets)),
        grid_spec=pltpu.PrefetchScalarGridSpec(num_scalar_prefetch=3, grid=(t//tt,),
            in_specs=[row(1), row(d), row(d), row(d)] + [pl.BlockSpec(memory_space=pl.ANY)]*len(rets) + [blk]*len(prev), out_specs=row(d),
            scratch_shapes=[pltpu.VMEM((n+16, 128), BF16), pltpu.VMEM((tt*16, 128), F32), pltpu.SemaphoreType.DMA((len(rets),))]),
        out_shape=jax.ShapeDtypeStruct((t, d), BF16), name="final",
        cost_estimate=pl.CostEstimate(flops=1024, bytes_accessed=2*n*128+24*t*d, transcendentals=0),
        compiler_params=pltpu.CompilerParams(dimension_semantics=("arbitrary",), vmem_limit_bytes=40<<20))(k, idx, w, zero, y, f, u, *rets, *prev)


def _rms(v, g):
    vf = v.astype(F32)
    return (vf * lax.rsqrt(jnp.mean(vf * vf, axis=-1, keepdims=True) + EPS) * g.astype(F32)).astype(BF16)


def _tables(pos):
    half = ROPE // 2
    ang = pos.astype(F32)[:, None] * (10000.0 ** (-jnp.arange(half, dtype=F32) / half))[None, :]
    cos, sin = jnp.cos(ang), jnp.sin(ang)
    z = jnp.zeros_like(sin)
    cat = lambda *a: jnp.concatenate(a, axis=1)
    return cat(cos, cos, z, z), cat(z, sin, z, z), cat(-sin, z, z, z)


def _after(v, *deps):
    return lax.optimization_barrier((v,) + deps)[0]


def solution(mesh):
    ncp = mesh.shape['cp']
    ngroup = mesh.shape['b'] * ncp
    axes = ('b', 'cp')
    tok = P(('dp', 'b'), 'cp', None)
    rep = P()
    espec = P(('b', 'cp'), None, None)

    def layer(x, ids, g_attn, w_q, w_dkv, w_kr, w_uk, w_uv, w_o, g_ffn, w_fg, w_fu, w_fd, g_moe, w_r, w_eg, w_eu, w_ed):
        rows, seq, d = x.shape
        top = ids.shape[-1]
        t = rows * seq
        epd = w_eg.shape[0]
        ne = epd * ngroup
        nslot = w_r.shape[1]
        hot = (nslot // top) // 2
        cap = (t + hot - 1) // hot
        i = lax.axis_index('cp')
        me = lax.axis_index('b') * ncp + i
        xt = x.reshape(t, d)
        tabs = _tables(i * seq + jnp.arange(seq))
        p = lax.axis_index('b')
        nb = ngroup // ncp
        idt = ids.reshape(t, top).T
        n, kv, logits, u = pre(xt, g_attn.reshape(1, d), g_moe.reshape(1, d), w_dkv, w_kr, w_r, tabs, 1)
        g = jax.nn.softmax(logits, axis=-1)
        oh = idt[:, :, None] == jnp.arange(nslot)
        sel = jnp.sum(jnp.where(oh, g[None], 0.0), axis=2)
        gate = sel / jnp.sum(sel, axis=0, keepdims=True)
        zero = jnp.sum(jnp.where(idt < ne, 0.0, gate), axis=0)
        meta = lax.all_gather(jnp.concatenate([idt.astype(F32), gate]), axes)
        meta, u = lax.optimization_barrier((meta, u))
        ua = lax.all_gather(u, axes)
        ida = meta[:, :top].astype(jnp.int32)

        def hop(v, *pairs):
            return lax.ppermute(v, 'b', list(pairs))

        far = lax.ppermute(kv, 'cp', [(0, 2), (1, 3)])
        near = lax.ppermute(kv, 'cp', [(0, 1), (2, 3)])
        kvs = [kv, far, near, lax.ppermute(far, 'cp', [(2, 3), (3, 2)])]
        home = [p] + [jnp.asarray(v, jnp.int32)[p] for v in ([3, 0, 3, 0], [2, 3, 0, 1], [1, 2, 1, 2])]
        k = jnp.arange(t)
        tri = (k[:, None] < k[None, :]).astype(BF16)
        hit = jnp.any(ida[:, None] == (epd * me + jnp.arange(epd))[None, :, None, None], axis=2)
        idl = jnp.stack([lax.dynamic_index_in_dim(ida, h * ncp + i, 0, keepdims=False) for h in home])
        gl = jnp.stack([lax.dynamic_index_in_dim(meta, h * ncp + i, 0, keepdims=False) for h in home])[:, top:]
        npl = epd * ncp
        x16 = idl - npl * p
        onp = (x16 >= 0) & (x16 < npl)
        ohl = x16[:, None] == jnp.arange(npl)[None, :, None, None]
        hitl = jnp.any(ohl, axis=2)
        both = jnp.concatenate([hit.reshape(-1, t), hitl.reshape(-1, t)]).astype(BF16)
        before = jnp.dot(both, tri, preferred_element_type=F32).astype(jnp.int32)
        rank = jnp.where(hit, before[:ngroup * epd].reshape(ngroup, epd, t), -1)
        some = jnp.any(hit, axis=2)
        rk = jnp.sum(jnp.where(ohl, before[ngroup * epd:].reshape(nb, npl, 1, t), 0), axis=1)
        nh = 2
        eh = epd // nh
        halved = x16 % epd // eh * (npl // nh) + x16 // epd * eh + x16 % eh
        xs = jnp.concatenate([x16[:1], halved[1:2], x16[2:]])
        row = jnp.where(onp, xs * cap + rk, npl * cap)
        wgt = jnp.where(onp, gl, 0.0)
        seen = jnp.cumsum(onp.astype(jnp.int32), axis=1)
        kmax = jnp.max(seen[:, -1], axis=1)
        put = onp[:, None] & (seen[:, None] - 1 == jnp.arange(top)[None, :, None, None])
        row = jnp.sum(jnp.where(put, row[:, None] - npl * cap, 0), axis=2) + npl * cap
        wgt = jnp.sum(jnp.where(put, wgt[:, None], 0.0), axis=2)
        def heads(k, dep):
            return attn(_after(i.reshape(1), dep), q, kvs, w_uv, k, 4)

        def rows_of(k, dep, parts=1):
            h = home[k]
            hs = _after(jnp.stack([h * ncp, h * ncp]), dep)
            xg = pick(hs, rank, ua, ncp, cap)
            full = lax.dynamic_slice_in_dim(some, h * ncp, ncp, 0)
            lst = jnp.argsort(~full, axis=0, stable=True).astype(jnp.int32).T.reshape(-1)
            num = jnp.sum(full, axis=0, dtype=jnp.int32)
            c = epd // parts
            outs = []
            for e in range(0, epd, c):
                outs.append(expert(e, c, _after(num, *outs), lst, xg, w_eg, w_eu, w_ed))
            return outs

        def back(k, outs):
            rets = []
            for o in outs:
                o = _after(o, *rets)
                rets.append(lax.all_to_all(o.reshape(ncp, -1, 128), 'cp', 0, 0).reshape(-1, 128))
            return jnp.maximum(kmax[k], 1).reshape(1), row[k].reshape(-1), wgt[k].reshape(-1), rets

        q = qproj(n, w_q, w_uk, tabs)
        oa = heads(0, q)
        ob = heads(1, oa)
        oc = heads(2, ob)
        o1 = rows_of(1, oc, 2)
        a1 = back(1, o1)
        od = heads(3, o1[-1])
        s1 = part(_after(a1[0], od), *a1[1:], [], t)
        r1 = hop(s1, (3, 2), (0, 1))
        o2 = rows_of(2, s1)
        a2 = back(2, o2)
        o3 = rows_of(3, o2[-1])
        o = _after(jnp.concatenate([oa, ob, oc, od], axis=1), o3[-1])
        a = jnp.dot(o, w_o, preferred_element_type=F32).astype(BF16)
        y = (xt.astype(F32) + a.astype(F32)).astype(BF16)
        o0 = rows_of(0, y)
        a3 = back(3, o3)
        z2 = _rms(_after(y, o0[-1]), g_ffn)
        hg = jax.nn.silu(jnp.dot(z2, w_fg, preferred_element_type=F32))
        s2 = part(_after(a2[0], hg), *a2[1:], [r1], t)
        r2a, r2b = hop(s2, (2, 1), (1, 2)), hop(s2, (3, 2), (0, 1))
        hid = (hg * jnp.dot(_after(z2, s2), w_fu, preferred_element_type=F32)).astype(BF16)
        s3 = part(_after(a3[0], hid), *a3[1:], [r2b], t)
        rc = hop(s1 + r2a, (1, 0), (2, 3))
        rd, re = hop(s3, (1, 2), (2, 1)), hop(s3, (0, 1), (3, 2))
        a0 = back(0, o0)
        f = jnp.dot(_after(hid, s3), w_fd, preferred_element_type=F32).astype(BF16)
        h = final(*a0, zero[:, None], y, f, u, [rc, rd, re])
        return h.reshape(rows, seq, d)

    return jax.shard_map(layer, mesh=mesh, in_specs=(tok, tok) + (rep,) * 13 + (espec,) * 3, out_specs=tok, check_vma=False)
```

```python
import functools

import jax
import jax.numpy as jnp
from jax import lax
from jax.experimental import pallas as pl
from jax.experimental.pallas import tpu as pltpu
from jax.sharding import PartitionSpec as P


F32 = jnp.float32
BF16 = jnp.bfloat16
EPS = 1e-6


NOPE, ROPE = 128, 64
SCALE=(NOPE+ROPE)**-0.5
LOG2E=1.4426950408889634


def _rope(v, c, sa, sb):
    return v*c + pltpu.roll(v, 32, 1)*sa + pltpu.roll(v, 96, 1)*sb


def _pre_body(x_ref, ga_ref, gm_ref, wc_ref, wk_ref, wr_ref, c_ref, sa_ref, sb_ref, n_ref, kv_ref, lg_ref, *u_refs):
    xf = x_ref[...].astype(F32)
    z = xf * lax.rsqrt(jnp.mean(xf*xf, axis=-1, keepdims=True) + EPS)
    n = (z * ga_ref[...].astype(F32)).astype(BF16)
    u = (z * gm_ref[...].astype(F32)).astype(BF16)
    n_ref[...] = n
    w = u.shape[1]//len(u_refs)
    for k, r in enumerate(u_refs): r[...] = u[:, k*w:(k+1)*w]
    r = wc_ref.shape[1]
    kv_ref[:, :r] = jnp.dot(n, wc_ref[...], preferred_element_type=F32).astype(BF16)
    kr = jnp.dot(n, wk_ref[...], preferred_element_type=F32)
    kr = jnp.concatenate([kr, jnp.zeros_like(kr)], axis=1)
    kv_ref[:, r:] = _rope(kr, c_ref[...], sa_ref[...], sb_ref[...]).astype(BF16)
    lg_ref[...] = jnp.dot(u, wr_ref[...], preferred_element_type=F32)


def pre(x, ga, gm, wc, wk, wr, tabs, nk, tm=256):
    t, d = x.shape
    r = wc.shape[1]
    row = lambda w: pl.BlockSpec((tm, w), lambda i: (i, 0))
    full = lambda a: pl.BlockSpec(a.shape, lambda i: (0,)*a.ndim)
    ns = wr.shape[1]
    return pl.pallas_call(_pre_body, grid=(t//tm,),
        in_specs=[row(d), full(ga), full(gm), full(wc), full(wk), full(wr), row(128), row(128), row(128)],
        out_specs=[row(d), row(r+128), row(ns)] + [row(d//nk)]*nk,
        out_shape=[jax.ShapeDtypeStruct((t, d), BF16), jax.ShapeDtypeStruct((t, r+128), BF16), jax.ShapeDtypeStruct((t, ns), F32)]
                  + [jax.ShapeDtypeStruct((t, d//nk), BF16)]*nk,
        name="pre", cost_estimate=pl.CostEstimate(flops=1024, bytes_accessed=6*t*d, transcendentals=0),
        compiler_params=pltpu.CompilerParams(dimension_semantics=("arbitrary",), vmem_limit_bytes=40<<20))(x, ga, gm, wc, wk, wr, *tabs)


def _qproj_body(n_ref, w_ref, uk_ref, c_ref, sa_ref, sb_ref, o_ref):
    q = jnp.dot(n_ref[...], w_ref[...], preferred_element_type=F32)
    t0, t1, t2 = q[:, :128], q[:, 128:256], q[:, 256:]
    r1, r2 = pltpu.roll(t1, 64, 1), pltpu.roll(t2, 64, 1)
    lane = lax.broadcasted_iota(jnp.int32, t0.shape, 1)
    nope = (t0, jnp.where(lane < 64, r1, r2))
    rope = (t1, r2)
    c, sa, sb = c_ref[...], sa_ref[...], sb_ref[...]
    r = uk_ref.shape[2]
    for k in range(2):
        o_ref[k, :, :r] = jnp.dot(nope[k].astype(BF16), uk_ref[k], preferred_element_type=F32).astype(BF16)
        o_ref[k, :, r:] = _rope(rope[k], c, sa, sb).astype(BF16)


def qproj(n, wq, wuk, tabs, tm=512):
    t, d = n.shape
    h, _, r = wuk.shape
    tab = pl.BlockSpec((tm, 128), lambda j, i: (i, 0))
    return pl.pallas_call(_qproj_body, grid=(h//2, t//tm),
        in_specs=[pl.BlockSpec((tm, d), lambda j, i: (i, 0)), pl.BlockSpec((d, 384), lambda j, i: (0, j)),
                  pl.BlockSpec((2, NOPE, r), lambda j, i: (j, 0, 0)), tab, tab, tab],
        out_specs=pl.BlockSpec((2, tm, r+128), lambda j, i: (j, i, 0)),
        out_shape=jax.ShapeDtypeStruct((h, t, r+128), BF16), name="qproj",
        cost_estimate=pl.CostEstimate(flops=1024, bytes_accessed=2*(h//2*t*d+d*h*192+t*h*(r+128)), transcendentals=0),
        compiler_params=pltpu.CompilerParams(dimension_semantics=("arbitrary","arbitrary"), vmem_limit_bytes=40<<20))(n, wq, wuk, *tabs)


def _attn_body(tq, sub, i_ref, q_ref, k0, k1, k2, k3, uv_ref, o_ref, m_ref, l_ref, acc_ref):
    at = i_ref[0]
    seq, r = q_ref.shape[1], uv_ref.shape[1]
    CF = SCALE*LOG2E
    nt = (((1,), (1,)), ((), ()))
    def block(rows, kv, diag, first):
        q = q_ref[0, rows:rows+sub]
        s = lax.dot_general(q, kv, nt, preferred_element_type=F32)
        if diag is not None:
            rr = lax.broadcasted_iota(jnp.int32, s.shape, 0) + diag
            cc = lax.broadcasted_iota(jnp.int32, s.shape, 1)
            s = jnp.where(rr >= cc, s, -jnp.inf)
        mx = jnp.max(s, axis=1, keepdims=True)
        if first:
            m = jnp.broadcast_to(mx, (sub, 128))
            p = jnp.exp2((s - mx)*CF)
            l_ref[rows:rows+sub] = jnp.broadcast_to(jnp.sum(p, axis=1, keepdims=True), (sub, 128))
            acc_ref[rows:rows+sub] = jnp.dot(p.astype(BF16), kv[:, :r], preferred_element_type=F32)
        else:
            m0 = m_ref[rows:rows+sub]
            m = jnp.maximum(m0, mx)
            corr = jnp.exp2((m0 - m)*CF)
            p = jnp.exp2((s - m[:, :1])*CF)
            l_ref[rows:rows+sub] = l_ref[rows:rows+sub]*corr + jnp.sum(p, axis=1, keepdims=True)
            acc_ref[rows:rows+sub] = acc_ref[rows:rows+sub]*corr[:, :1] + jnp.dot(p.astype(BF16), kv[:, :r], preferred_element_type=F32)
        m_ref[rows:rows+sub] = m
    for t0 in range(0, seq, tq):
        for rows in range(t0, t0+tq, sub):
            block(rows, k0[:t0+tq], rows, True)
    for ok, kr in ((at >= 2, k1), (lax.rem(at, 2) == 1, k2), (at >= 2, k3)):
        @pl.when(ok)
        def _():
            for rows in range(0, seq, sub):
                block(rows, kr[...], None, False)
    for rows in range(0, seq, 256):
        lat = (acc_ref[rows:rows+256] / l_ref[rows:rows+256, :1]).astype(BF16)
        o_ref[rows:rows+256] = jnp.dot(lat, uv_ref[0], preferred_element_type=F32).astype(BF16)


def attn(i, q, kvs, wuv, part, parts, tq=512, sub=512):
    h, t, w = q.shape
    r, vd = wuv.shape[1:]
    hp = h // parts
    o = part * hp
    kspec = pl.BlockSpec((t, w), lambda j, *_: (0, 0), pipeline_mode=pl.Buffered(1))
    return pl.pallas_call(functools.partial(_attn_body, tq, sub),
        grid_spec=pltpu.PrefetchScalarGridSpec(num_scalar_prefetch=1, grid=(hp,),
            in_specs=[pl.BlockSpec((1, t, w), lambda j, *_: (j + o, 0, 0)), kspec, kspec, kspec, kspec,
                      pl.BlockSpec((1, r, vd), lambda j, *_: (j + o, 0, 0))],
            out_specs=pl.BlockSpec((t, vd), lambda j, *_: (0, j)),
            scratch_shapes=[pltpu.VMEM((t, 128), F32), pltpu.VMEM((t, 128), F32), pltpu.VMEM((t, r), F32)]),
        out_shape=jax.ShapeDtypeStruct((t, hp*vd), BF16), name="attn",
        cost_estimate=pl.CostEstimate(flops=1024, bytes_accessed=2*hp*t*w, transcendentals=hp*t*t*5//2),
        compiler_params=pltpu.CompilerParams(dimension_semantics=("arbitrary",), vmem_limit_bytes=60<<20))(i, q, *kvs, wuv)


def _pick_body(h_ref, rank_ref, u_ref, o_ref):
    ne, cap = o_ref.shape[0], o_ref.shape[2]
    t = u_ref.shape[1]
    row = lax.broadcasted_iota(jnp.int32, (cap, t), 0)
    oh = jnp.concatenate([(rank_ref[0, e:e+1, :] == row).astype(F32).astype(BF16) for e in range(ne)], axis=0)
    o = jnp.dot(oh, u_ref[0], preferred_element_type=F32).astype(BF16)
    for e in range(ne):
        o_ref[e, 0] = o[e*cap:(e+1)*cap]


def pick(h, rank, u, nl, cap):
    _, E, t = rank.shape
    d = u.shape[-1]
    return pl.pallas_call(
        _pick_body,
        grid_spec=pltpu.PrefetchScalarGridSpec(num_scalar_prefetch=1, grid=(nl,),
            in_specs=[pl.BlockSpec((1, E, t), lambda s, h: (h[0] + s, 0, 0)), pl.BlockSpec((1, t, d), lambda s, h: (h[1] + s, 0, 0))],
            out_specs=pl.BlockSpec((E, 1, cap, d), lambda s, h: (0, s, 0, 0))),
        out_shape=jax.ShapeDtypeStruct((E, nl, cap, d), BF16), name="pick",
        cost_estimate=pl.CostEstimate(flops=1024, bytes_accessed=2*nl*(t+E*cap)*d, transcendentals=0),
        compiler_params=pltpu.CompilerParams(dimension_semantics=("arbitrary",), vmem_limit_bytes=40<<20))(h, rank, u)


def _expert_body(e0, ne, n_ref, lst_ref, x_hbm, wg_hbm, wu_hbm, wd_hbm, o_hbm,
                 x_ref, w_ref, wd_ref, hid_ref, f_ref, ob_ref, xsem, wsem, dsem, osem):
    _, S, cap, d = x_hbm.shape
    ff = wg_hbm.shape[-1]
    kc = d // 4
    half = S // 2
    tm = half * cap
    def wcopies(e):
        b = e % 2
        out = []
        for i in range(4):
            out.append(pltpu.make_async_copy(wg_hbm.at[e, pl.ds(i*kc, kc)], w_ref.at[b, pl.ds(i*kc, kc), pl.ds(0, ff)], wsem.at[b, 0, i]))
            out.append(pltpu.make_async_copy(wu_hbm.at[e, pl.ds(i*kc, kc)], w_ref.at[b, pl.ds(i*kc, kc), pl.ds(ff, ff)], wsem.at[b, 1, i]))
        return out
    def dcopy(e):
        return pltpu.make_async_copy(wd_hbm.at[e], wd_ref.at[e % 2], dsem.at[e % 2])
    def xcopies(e):
        return [pltpu.make_async_copy(x_hbm.at[e, lst_ref[e*S + j]], x_ref.at[e % 2, pl.ds(j*cap, cap)], xsem.at[e % 2, j]) for j in range(S)]
    def ocopies(e, m):
        out = []
        for j in range(half):
            s = lst_ref[e*S + m*half + j]
            out.append(pltpu.make_async_copy(ob_ref.at[m, pl.ds(j*cap*16, cap*16)], o_hbm.at[pl.ds((s*ne + e - e0)*cap*16, cap*16)], osem.at[m, j]))
        return out
    def when(e, m):
        return n_ref[e] > m*half
    def load(e):
        @pl.when(when(e, 0))
        def _():
            for c in wcopies(e): c.start()
            for c in xcopies(e): c.start()
            dcopy(e).start()
    def out_wait(e, m):
        @pl.when(when(e, m))
        def _():
            for c in ocopies(e, m): c.wait()
    load(e0)
    for e in range(e0, e0 + ne):
        b = e % 2
        if e + 1 < e0 + ne:
            load(e + 1)
        @pl.when(when(e, 0))
        def _():
            for c in xcopies(e): c.wait()
            for c in wcopies(e): c.wait()
        for m in range(2):
            if e > e0:
                out_wait(e - 1, m)
            @pl.when(when(e, m))
            def _():
                gu = jnp.dot(x_ref[b, m*tm:(m+1)*tm], w_ref[b], preferred_element_type=F32)
                g, u = gu[:, :ff], gu[:, ff:]
                hid_ref[...] = (g * jax.nn.sigmoid(g) * u).astype(BF16)
                if m == 0:
                    dcopy(e).wait()
                for c0 in range(0, d, 1024):
                    o = jnp.dot(hid_ref[...], wd_ref[b, :, c0:c0+1024], preferred_element_type=F32)
                    for k in range(0, 1024, 128):
                        f_ref[pl.ds((c0+k)//128, tm, stride=16), :] = o[:, k:k+128]
                ob_ref[m] = f_ref[...].astype(BF16)
                for c in ocopies(e, m): c.start()
    for m in range(2):
        out_wait(e0 + ne - 1, m)


def expert(e0, ne, n, lst, xg, wg, wu, wd):
    E, S, cap, d = xg.shape
    ff = wg.shape[-1]
    tm = S // 2 * cap
    any_ = pl.BlockSpec(memory_space=pl.ANY)
    return pl.pallas_call(
        functools.partial(_expert_body, e0, ne),
        grid_spec=pltpu.PrefetchScalarGridSpec(num_scalar_prefetch=2, grid=(), in_specs=[any_]*4, out_specs=any_,
            scratch_shapes=[pltpu.VMEM((2, S*cap, d), BF16), pltpu.VMEM((2, d, 2*ff), BF16), pltpu.VMEM((2, ff, d), BF16),
                            pltpu.VMEM((tm, ff), BF16), pltpu.VMEM((tm*16, 128), F32), pltpu.VMEM((2, tm*16, 128), BF16),
                            pltpu.SemaphoreType.DMA((2, S)), pltpu.SemaphoreType.DMA((2, 2, 4)), pltpu.SemaphoreType.DMA((2,)),
                            pltpu.SemaphoreType.DMA((2, S//2))]),
        out_shape=jax.ShapeDtypeStruct((S*ne*cap*16, 128), BF16), name="expert",
        cost_estimate=pl.CostEstimate(flops=1024, bytes_accessed=6*E*d*ff+4*E*S*cap*d, transcendentals=E*S*cap*ff),
        compiler_params=pltpu.CompilerParams(vmem_limit_bytes=62<<20))(n, lst, xg, wg, wu, wd)


def _rows(k_ref, idx_ref, w_ref, r_refs, buf, scr, sem, tt):
    n = buf.shape[0] - 16
    m = n // len(r_refs)
    i = pl.program_id(0)
    t = pl.num_programs(0)*tt
    @pl.when(i == 0)
    def _():
        cs = [pltpu.make_async_copy(r, buf.at[pl.ds(c*m, m)], sem.at[c]) for c, r in enumerate(r_refs)]
        for c in cs: c.start()
        buf[n:n+16] = jnp.zeros((16, 128), BF16)
        for c in cs: c.wait()
    def row(j, q):
        g = j*t + i*tt + q
        return w_ref[g]*buf[pl.ds(pl.multiple_of(idx_ref[g]*16, 16), 16), :].astype(F32)
    def first(q, _):
        scr[pl.ds(pl.multiple_of(q*16, 16), 16), :] = row(0, q)
        return 0
    lax.fori_loop(0, tt, first, 0, unroll=8)
    def more(j, _):
        def add(q, _):
            s = pl.ds(pl.multiple_of(q*16, 16), 16)
            scr[s, :] = scr[s, :] + row(j, q)
            return 0
        lax.fori_loop(0, tt, add, 0, unroll=8)
        return 0
    lax.fori_loop(1, k_ref[0], more, 0)


def _part_body(nr, k_ref, idx_ref, w_ref, *rest):
    r_refs, (*prev, o_ref, buf, sem) = rest[:nr], rest[nr:]
    _rows(k_ref, idx_ref, w_ref, r_refs, buf, o_ref, sem, o_ref.shape[0]//16)
    for p in prev:
        o_ref[...] += p[...]


def part(k, idx, w, rets, prev, t, tt=128):
    n = sum(r.shape[0] for r in rets)
    blk = pl.BlockSpec((tt*16, 128), lambda i, *_: (i, 0))
    return pl.pallas_call(functools.partial(_part_body, len(rets)),
        grid_spec=pltpu.PrefetchScalarGridSpec(num_scalar_prefetch=3, grid=(t//tt,),
            in_specs=[pl.BlockSpec(memory_space=pl.ANY)]*len(rets) + [blk]*len(prev), out_specs=blk,
            scratch_shapes=[pltpu.VMEM((n+16, 128), BF16), pltpu.SemaphoreType.DMA((len(rets),))]),
        out_shape=jax.ShapeDtypeStruct((t*16, 128), F32), name="part",
        cost_estimate=pl.CostEstimate(flops=1024, bytes_accessed=2*n*128+12*t*2048, transcendentals=0),
        compiler_params=pltpu.CompilerParams(dimension_semantics=("arbitrary",), vmem_limit_bytes=40<<20))(k, idx, w, *rets, *prev)


def _final_body(nr, k_ref, idx_ref, w_ref, z_ref, y_ref, f_ref, u_ref, *rest):
    r_refs, (*prev, h_ref, buf, scr, sem) = rest[:nr], rest[nr:]
    tt = y_ref.shape[0]
    _rows(k_ref, idx_ref, w_ref, r_refs, buf, scr, sem, tt)
    for p in prev:
        scr[...] += p[...]
    z = z_ref[...]
    for k in range(16):
        c = slice(k*128, (k+1)*128)
        m = scr[pl.ds(k, tt, stride=16), :] + z*u_ref[:, c].astype(F32)
        h_ref[:, c] = (y_ref[:, c].astype(F32) + f_ref[:, c].astype(F32) + m).astype(BF16)


def final(k, idx, w, rets, zero, y, f, u, prev, tt=128):
    t, d = y.shape
    n = sum(r.shape[0] for r in rets)
    row = lambda c: pl.BlockSpec((tt, c), lambda i, *_: (i, 0))
    blk = pl.BlockSpec((tt*16, 128), lambda i, *_: (i, 0))
    return pl.pallas_call(functools.partial(_final_body, len(rets)),
        grid_spec=pltpu.PrefetchScalarGridSpec(num_scalar_prefetch=3, grid=(t//tt,),
            in_specs=[row(1), row(d), row(d), row(d)] + [pl.BlockSpec(memory_space=pl.ANY)]*len(rets) + [blk]*len(prev), out_specs=row(d),
            scratch_shapes=[pltpu.VMEM((n+16, 128), BF16), pltpu.VMEM((tt*16, 128), F32), pltpu.SemaphoreType.DMA((len(rets),))]),
        out_shape=jax.ShapeDtypeStruct((t, d), BF16), name="final",
        cost_estimate=pl.CostEstimate(flops=1024, bytes_accessed=2*n*128+24*t*d, transcendentals=0),
        compiler_params=pltpu.CompilerParams(dimension_semantics=("arbitrary",), vmem_limit_bytes=40<<20))(k, idx, w, zero, y, f, u, *rets, *prev)


def _rms(v, g):
    vf = v.astype(F32)
    return (vf * lax.rsqrt(jnp.mean(vf * vf, axis=-1, keepdims=True) + EPS) * g.astype(F32)).astype(BF16)


def _tables(pos):
    half = ROPE // 2
    ang = pos.astype(F32)[:, None] * (10000.0 ** (-jnp.arange(half, dtype=F32) / half))[None, :]
    cos, sin = jnp.cos(ang), jnp.sin(ang)
    z = jnp.zeros_like(sin)
    cat = lambda *a: jnp.concatenate(a, axis=1)
    return cat(cos, cos, z, z), cat(z, sin, z, z), cat(-sin, z, z, z)


def _after(v, *deps):
    return lax.optimization_barrier((v,) + deps)[0]


def solution(mesh):
    ncp = mesh.shape['cp']
    ngroup = mesh.shape['b'] * ncp
    axes = ('b', 'cp')
    tok = P(('dp', 'b'), 'cp', None)
    rep = P()
    espec = P(('b', 'cp'), None, None)

    def layer(x, ids, g_attn, w_q, w_dkv, w_kr, w_uk, w_uv, w_o, g_ffn, w_fg, w_fu, w_fd, g_moe, w_r, w_eg, w_eu, w_ed):
        rows, seq, d = x.shape
        top = ids.shape[-1]
        t = rows * seq
        epd = w_eg.shape[0]
        ne = epd * ngroup
        nslot = w_r.shape[1]
        hot = (nslot // top) // 2
        cap = (t + hot - 1) // hot
        i = lax.axis_index('cp')
        me = lax.axis_index('b') * ncp + i
        xt = x.reshape(t, d)
        tabs = _tables(i * seq + jnp.arange(seq))
        p = lax.axis_index('b')
        nb = ngroup // ncp
        idt = ids.reshape(t, top).T
        n, kv, logits, u = pre(xt, g_attn.reshape(1, d), g_moe.reshape(1, d), w_dkv, w_kr, w_r, tabs, 1)
        g = jax.nn.softmax(logits, axis=-1)
        oh = idt[:, :, None] == jnp.arange(nslot)
        sel = jnp.sum(jnp.where(oh, g[None], 0.0), axis=2)
        gate = sel / jnp.sum(sel, axis=0, keepdims=True)
        zero = jnp.sum(jnp.where(idt < ne, 0.0, gate), axis=0)
        meta = lax.all_gather(jnp.concatenate([idt.astype(F32), gate]), axes)
        meta, u = lax.optimization_barrier((meta, u))
        ua = lax.all_gather(u, axes)
        ida = meta[:, :top].astype(jnp.int32)

        def hop(v, *pairs):
            return lax.ppermute(v, 'b', list(pairs))

        far = lax.ppermute(kv, 'cp', [(0, 2), (1, 3)])
        near = lax.ppermute(kv, 'cp', [(0, 1), (2, 3)])
        kvs = [kv, far, near, lax.ppermute(far, 'cp', [(2, 3), (3, 2)])]
        home = [p] + [jnp.asarray(v, jnp.int32)[p] for v in ([3, 0, 3, 0], [2, 3, 0, 1], [1, 2, 1, 2])]
        k = jnp.arange(t)
        tri = (k[:, None] < k[None, :]).astype(BF16)
        hit = jnp.any(ida[:, None] == (epd * me + jnp.arange(epd))[None, :, None, None], axis=2)
        idl = jnp.stack([lax.dynamic_index_in_dim(ida, h * ncp + i, 0, keepdims=False) for h in home])
        gl = jnp.stack([lax.dynamic_index_in_dim(meta, h * ncp + i, 0, keepdims=False) for h in home])[:, top:]
        npl = epd * ncp
        x16 = idl - npl * p
        onp = (x16 >= 0) & (x16 < npl)
        ohl = x16[:, None] == jnp.arange(npl)[None, :, None, None]
        hitl = jnp.any(ohl, axis=2)
        both = jnp.concatenate([hit.reshape(-1, t), hitl.reshape(-1, t)]).astype(BF16)
        before = jnp.dot(both, tri, preferred_element_type=F32).astype(jnp.int32)
        rank = jnp.where(hit, before[:ngroup * epd].reshape(ngroup, epd, t), -1)
        some = jnp.any(hit, axis=2)
        rk = jnp.sum(jnp.where(ohl, before[ngroup * epd:].reshape(nb, npl, 1, t), 0), axis=1)
        nh = 2
        eh = epd // nh
        halved = x16 % epd // eh * (npl // nh) + x16 // epd * eh + x16 % eh
        xs = jnp.concatenate([x16[:1], halved[1:2], x16[2:]])
        row = jnp.where(onp, xs * cap + rk, npl * cap)
        wgt = jnp.where(onp, gl, 0.0)
        seen = jnp.cumsum(onp.astype(jnp.int32), axis=1)
        kmax = jnp.max(seen[:, -1], axis=1)
        put = onp[:, None] & (seen[:, None] - 1 == jnp.arange(top)[None, :, None, None])
        row = jnp.sum(jnp.where(put, row[:, None] - npl * cap, 0), axis=2) + npl * cap
        wgt = jnp.sum(jnp.where(put, wgt[:, None], 0.0), axis=2)
        def heads(k, dep):
            return attn(_after(i.reshape(1), dep), q, kvs, w_uv, k, 4)

        def rows_of(k, dep, parts=1):
            h = home[k]
            hs = _after(jnp.stack([h * ncp, h * ncp]), dep)
            xg = pick(hs, rank, ua, ncp, cap)
            full = lax.dynamic_slice_in_dim(some, h * ncp, ncp, 0)
            lst = jnp.argsort(~full, axis=0, stable=True).astype(jnp.int32).T.reshape(-1)
            num = jnp.sum(full, axis=0, dtype=jnp.int32)
            c = epd // parts
            outs = []
            for e in range(0, epd, c):
                outs.append(expert(e, c, _after(num, *outs), lst, xg, w_eg, w_eu, w_ed))
            return outs

        def back(k, outs):
            rets = []
            for o in outs:
                o = _after(o, *rets)
                rets.append(lax.all_to_all(o.reshape(ncp, -1, 128), 'cp', 0, 0).reshape(-1, 128))
            return jnp.maximum(kmax[k], 1).reshape(1), row[k].reshape(-1), wgt[k].reshape(-1), rets

        q = qproj(n, w_q, w_uk, tabs)
        oa = heads(0, q)
        ob = heads(1, oa)
        oc = heads(2, ob)
        od = heads(3, oc)
        o1 = rows_of(1, od, 2)
        a1 = back(1, o1)
        o = _after(jnp.concatenate([oa, ob, oc, od], axis=1), o1[-1])
        a = jnp.dot(o, w_o, preferred_element_type=F32).astype(BF16)
        y = (xt.astype(F32) + a.astype(F32)).astype(BF16)
        s1 = part(_after(a1[0], y), *a1[1:], [], t)
        r1 = hop(s1, (3, 2), (0, 1))
        o2 = rows_of(2, s1)
        a2 = back(2, o2)
        o3 = rows_of(3, o2[-1])
        o0 = rows_of(0, o3[-1])
        s2 = part(_after(a2[0], o0[-1]), *a2[1:], [r1], t)
        r2a, r2b = hop(s2, (2, 1), (1, 2)), hop(s2, (3, 2), (0, 1))
        a3 = back(3, [_after(o3[-1], s2)])
        z2 = _rms(_after(y, s2), g_ffn)
        hg = jax.nn.silu(jnp.dot(z2, w_fg, preferred_element_type=F32))
        hid = (hg * jnp.dot(_after(z2, hg), w_fu, preferred_element_type=F32)).astype(BF16)
        s3 = part(_after(a3[0], hid), *a3[1:], [r2b], t)
        rc = hop(s1 + r2a, (1, 0), (2, 3))
        rd, re = hop(s3, (1, 2), (2, 1)), hop(s3, (0, 1), (3, 2))
        a0 = back(0, [_after(o0[-1], s3)])
        f = jnp.dot(_after(hid, s3), w_fd, preferred_element_type=F32).astype(BF16)
        h = final(*a0, zero[:, None], y, f, u, [rc, rd, re])
        return h.reshape(rows, seq, d)

    return jax.shard_map(layer, mesh=mesh, in_specs=(tok, tok) + (rep,) * 13 + (espec,) * 3, out_specs=tok, check_vma=False)
```
